32 devices in a mesh: ang: 8 (over z, x), tile: 4 (over y, core).
Axes of the slice: x: 2, y: 2, z: 4, core: 2. Of those that a mesh axis runs over, the one named last changes fastest.
Arguments:
- sinogram: float32 [2, 64, 2048], P(None, 'ang'), may hold values from -6 to 6
- ray_offsets: int32 [64, 256], P('ang'), may hold values from 0 to 2047
- merge_matrices: float32 [3, 2, 2, 256, 256], replicated, may hold values from -1 to 1.5, as said below
Outputs:
- reconstruction: float32 [2, 2048, 2048], P(None, 'ang')
The draws below stay inside these ranges and needn't reach their ends.
Inputs may be any that keep to these rules, and one draw needn't show every extreme that they name: merge_matrices[l, b, k] is zero outside the columns b * (96) to b * 96 + 256 / 2 + 31.
All inputs are finite; a program needn't handle non-finite values.
Results may differ from the reference program's by a relative error of at most 0.0003.
Values sent between devices are 32-bit elements; how exact they have to be, the bound alone decides.
No kernel may reach another device: no remote copies, remote signals or barrier semaphores. Data moves between devices by JAX's collectives and lax.ppermute only.
A program may use at most 768 MiB of HBM per device.

```python
import math
import jax
import jax.numpy as jnp
from jax import lax

NPIX = 2048
ANG_DEV = 8
SLICES = 2
ANGLES = 64
R = 256
HALO = 32
LEVELS = 3
N_ANG = 8


def draw_merge_matrices(key, part):
    shape = (LEVELS, 2, 2, R, R)
    noise = jnp.clip(jax.random.normal(key, shape, jnp.float32), -4.0, 4.0)
    width = R // 2 + HALO
    fine = jnp.arange(R, dtype=jnp.float32)[None, :, None]
    coarse = jnp.arange(R, dtype=jnp.float32)[None, None, :]
    half_bit = jnp.arange(2, dtype=jnp.float32)[:, None, None]
    centre = half_bit * (R // 2) + 0.5 * fine
    kernel = jnp.maximum(0.0, 1.0 - jnp.abs(coarse - centre))
    low_col = half_bit * (R // 2 - HALO)
    inside = jnp.logical_and(coarse >= low_col, coarse < low_col + width).astype(jnp.float32)
    kernel = kernel[None, :, None, :, :]
    inside = inside[None, :, None, :, :]
    return inside * (0.5 * kernel + 0.5 * noise / math.sqrt(width))


def set_ends(values, stream_key, smallest, largest):
    longest = values.shape.index(max(values.shape))
    spots = []
    for shift in (0, 1):
        where = [jax.random.randint(jax.random.fold_in(stream_key, axis), (), 0, length) for axis, length in enumerate(values.shape)]
        where[longest] = (where[longest] + shift) % values.shape[longest]
        spots.append(tuple(where))
    return values.at[spots[0]].set(smallest).at[spots[1]].set(largest)


def level_of(own_key, dims, cuts, smallest, largest):
    def one(position, parts):
        draws = jax.random.uniform(jax.random.fold_in(jax.random.fold_in(own_key, 6), position), (parts,), jnp.float32, smallest / len(cuts), largest / len(cuts))
        return jnp.repeat(jnp.exp(draws), dims[position] // parts).reshape((-1,) + (1,) * (len(dims) - position - 1))

    gain = one(*cuts[0])
    for cut in cuts[1:]:
        gain = gain * one(*cut)
    return gain


def scatter_about(key, dims, scale, bound, pieces=(), kind=jnp.bfloat16):
    entries = jax.random.normal(key, dims, jnp.float32) * scale
    if len(pieces) > 0:
        entries = level_of(key, dims, pieces, -0.22, 0.18) * entries
    return jnp.clip(entries, min=-bound, max=bound).astype(kind)


def setup_inputs(seed: int = 0) -> dict:
    splits = jax.random.split(jax.random.key(seed), 4)
    sinogram = scatter_about(splits[0], (SLICES, ANGLES, NPIX), 1.0, 6.0, ((1, 8),), jnp.float32)
    ray_offsets = set_ends(jax.random.randint(splits[1], (ANGLES, R), 0, NPIX), jax.random.fold_in(splits[1], 1), 0, NPIX - 1).astype(jnp.int32)
    merge_matrices = draw_merge_matrices(jax.random.fold_in(splits[3], 71), 0)
    return dict(sinogram=sinogram, ray_offsets=ray_offsets, merge_matrices=merge_matrices)


def apply_rows(matrix, field):
    return jnp.einsum('rk,...kw->...rw', matrix, field, precision=lax.Precision.HIGHEST)

def smear_rows(sinogram, offsets, columns):
    slices = sinogram.shape[0]
    angles = sinogram.shape[1]
    bin_count = sinogram.shape[2]
    row_count = offsets.shape[1]
    blocks = angles // 8
    grouped = sinogram.reshape(slices, blocks, 8, bin_count).transpose(1, 0, 2, 3)
    grouped_offsets = offsets.reshape(blocks, 8, row_count)
    angle_ids = jnp.arange(8, dtype=jnp.int32)[:, None, None]

    def add_block(running, inputs):
        rows_block, offset_block = inputs
        bin_index = jnp.remainder(columns[None, None, :] + offset_block[:, :, None], bin_count).astype(jnp.int32)
        samples = rows_block[:, angle_ids, bin_index]
        return (running + lax.optimization_barrier(jnp.sum(samples, axis=1)), None)
    zeros_init = jnp.zeros((slices, row_count, columns.shape[0]), jnp.float32)
    running, _ = lax.scan(add_block, zeros_init, (grouped, grouped_offsets))
    return running / math.sqrt(angles)

def reference(sinogram, ray_offsets, merge_matrices):
    grouped = sinogram.reshape(SLICES, N_ANG, ANG_DEV, NPIX).transpose(1, 0, 2, 3)
    offsets_grouped = ray_offsets.reshape(N_ANG, ANG_DEV, R)
    columns = jnp.arange(NPIX, dtype=jnp.int32)
    partial_value = lax.map(lambda inputs: smear_rows(inputs[0], inputs[1], columns), (grouped, offsets_grouped))
    for level_num in range(LEVELS):
        half_span = 2 ** (LEVELS - 1 - level_num)
        shaped = partial_value.reshape(N_ANG // (2 * half_span), 2, half_span, SLICES, R, NPIX)
        lower = shaped[:, 0]
        upper = shaped[:, 1]
        mats = merge_matrices[level_num]
        new_lower = apply_rows(mats[0, 0], lower) + apply_rows(mats[0, 1], upper)
        new_upper = apply_rows(mats[1, 0], upper) + apply_rows(mats[1, 1], lower)
        partial_value = jnp.stack([new_lower, new_upper], axis=1).reshape(N_ANG, SLICES, R, NPIX)
    return partial_value.transpose(1, 0, 2, 3).reshape(SLICES, NPIX, NPIX)
```

```python
import functools
import math

import jax
import jax.numpy as jnp
from jax import lax
from jax.experimental import pallas as pl
from jax.experimental.pallas import tpu as pltpu
from jax.sharding import PartitionSpec as P

LANES = 128
SUBLANES = 8


def packed_rows(sinogram, ray_offsets):
    slices, angles, bin_count = sinogram.shape
    rows = ray_offsets.shape[1]
    half = angles // 2
    run = slices * bin_count // LANES
    fields = sinogram.reshape(slices, 2, half, bin_count // run, run).transpose(1, 2, 4, 0, 3)
    fields = fields.reshape(2, half * run, LANES)
    words = ray_offsets.astype(jnp.float32).reshape(2, half, SUBLANES, rows // SUBLANES)
    words = words.transpose(0, 2, 1, 3).reshape(2, SUBLANES, -1)
    words = jnp.pad(words, ((0, 0), (0, 0), (0, LANES - words.shape[2])))
    return jnp.concatenate([fields, words], axis=1)


def split(value):
    high = value.astype(jnp.bfloat16)
    return high, (value - high.astype(jnp.float32)).astype(jnp.bfloat16)


def dot(left, right):
    return jnp.dot(left, right, preferred_element_type=jnp.float32)


class Smear:
    def __init__(self, half, slices, run, unroll, band, band_blocks, lines, staged, words, shift, tables):
        self.half, self.slices, self.run, self.unroll = half, slices, run, unroll
        self.band, self.band_blocks = band, band_blocks
        self.lines, self.staged, self.words, self.shift, self.tables = lines, staged, words, shift, tables
        self.lane_blocks = LANES // slices
        self.table_rows = (self.lane_blocks + 1) * run
        self.angles = 2 * half

    def put(self, place, part, source):
        size = self.half * self.run
        high, low = split(source[:size, :])
        where = pl.ds(pl.multiple_of((place * 2 + part) * size, size), size)
        self.lines[where, :LANES] = high
        self.lines[where, LANES:] = low
        where = pl.multiple_of((place * 2 + part) * SUBLANES, SUBLANES)
        self.staged[pl.ds(where, SUBLANES), :] = source[size:, :].astype(jnp.int32)

    def shift_matrices(self):
        line = lax.broadcasted_iota(jnp.int32, (2 * LANES, LANES), 0)
        lane = lax.broadcasted_iota(jnp.int32, (2 * LANES, LANES), 1)
        same = ((line // self.lane_blocks) % self.slices) == lane // self.lane_blocks
        distance = jnp.where(same, (line - lane) & (self.lane_blocks - 1), -1)
        for m in range(self.lane_blocks):
            self.shift[:, m * LANES : (m + 1) * LANES] = jnp.where(distance == m, 1.0, 0.0).astype(jnp.bfloat16)

    def build(self, place, table, first, count):
        size = self.angles * self.run
        lines = self.lines[place * size : (place + 1) * size, :]
        for m in range(count):
            columns = pl.ds(pl.multiple_of((first + m) * (2 * LANES), 2 * LANES), 2 * LANES)
            shifted = dot(lines, self.shift[:, columns])
            for a in range(self.angles):
                for n in range(2):
                    block = shifted[a * self.run : (a + 1) * self.run, n * LANES : (n + 1) * LANES]
                    start = pl.multiple_of((first + m) * (2 * self.run), SUBLANES)
                    table[pl.ds(start + (a * self.table_rows + n * self.run), self.run), :] = block

    def close(self, table):
        for a in range(self.angles):
            start = a * self.table_rows
            last = start + self.lane_blocks * self.run
            table[last : last + self.run, :] = table[start : start + self.run, :]

    def gather(self, place, table, step, partial, pitch, first, last):
        word_row = place * (2 * SUBLANES) + self.band + step
        first_sample = (place * self.band_blocks + step) * self.unroll
        vectors = self.run // SUBLANES
        for u in range(first, last):
            sums = [None] * vectors
            for a in range(self.angles):
                offset = self.words[word_row + (a // self.half) * SUBLANES, (a % self.half) * self.unroll + u]
                for n in range(vectors):
                    piece = table[pl.ds(offset + (a * self.table_rows + n * SUBLANES), SUBLANES), :]
                    sums[n] = piece if sums[n] is None else sums[n] + piece
            for n in range(vectors):
                start = first_sample + (u + n * SUBLANES * pitch)
                partial[pl.ds(start, SUBLANES, stride=pitch), :] = sums[n]

    def run_groups(self, count, partial, pitch):
        pairs = self.lane_blocks // 2
        share = -(-pairs // self.band_blocks)

        def first_step(step, carry):
            self.build(0, self.tables[0], jnp.minimum(step * share, pairs - share), share)
            return carry

        lax.fori_loop(0, self.band_blocks, first_step, 0)
        self.close(self.tables[0])
        for place in range(count):
            now, later = self.tables[place % 2], self.tables[(place + 1) % 2]

            def merged_step(step, carry):
                self.gather(place, now, step, partial, pitch, 0, self.unroll)
                return carry

            lax.fori_loop(0, self.band_blocks, merged_step, 0)
            if place + 1 < count:
                self.build(place + 1, later, 0, pairs)
                self.close(later)


def matrices_kernel(levels, width, angles, place_ref, all_ref, high_ref, low_ref, pair_ref, sems):
    copies = []
    for level in range(levels):
        own_bit = (place_ref[2] >> (levels - 1 - level)) & 1
        copies.append(pltpu.make_async_copy(all_ref.at[level, own_bit], pair_ref.at[level], sems.at[level]))
        copies[-1].start()
    rows = pair_ref.shape[2]
    scale = 1.0 / math.sqrt(angles)
    product = None
    for level in reversed(range(levels)):
        copies[level].wait()
        pair = [pair_ref[level, n] for n in range(2)]
        if level == 0:
            upper = place_ref[1] > 0
            pair = [jnp.where(upper, m[:, rows - width :], m[:, :width]) * scale for m in pair]
        if product is None:
            product = pair
            continue
        pair = [split(m) for m in pair]
        left = [split(m) for m in product]
        product = [
            dot(high, other_low) + dot(low, other_high) + dot(high, other_high)
            for other_high, other_low in pair
            for high, low in left
        ]
    high_ref[...], low_ref[...] = split(jnp.concatenate(product, axis=1))


def early_kernel(smear_sizes, pitch, place_ref, own_ref, neighbour_ref,
                 early_ref, lines_ref, staged_ref, words_ref, shift_ref, table_a, table_b, sem):
    half, slices, run, unroll, band_blocks = smear_sizes
    smear = Smear(half, slices, run, unroll, place_ref[1], band_blocks, lines_ref, staged_ref, words_ref, shift_ref, (table_a, table_b))
    for part in range(2):
        smear.put(0, part, own_ref.at[part])
        smear.put(1, part, neighbour_ref.at[part])
    copy = pltpu.make_async_copy(staged_ref, words_ref, sem)
    copy.start()
    smear.shift_matrices()
    copy.wait()
    smear.run_groups(2, early_ref, pitch)


def image_kernel(smear_sizes, size, width, early_pitch, pitch, turn_pitch, place_ref, *refs):
    early_ref, high_ref, low_ref = refs[size - 2 : size + 1]
    (out_ref, lines_ref, staged_ref, words_ref, shift_ref, table_a, table_b, partial_ref, turned_ref, sem) = refs[size + 1 :]
    half, slices, run, unroll, band_blocks = smear_sizes
    core = place_ref[0]
    smear = Smear(half, slices, run, unroll, place_ref[1], band_blocks, lines_ref, staged_ref, words_ref, shift_ref, (table_a, table_b))
    lane_blocks = smear.lane_blocks
    rows = out_ref.shape[1]
    for pair in range(size // 2 - 1):
        for group in range(2):
            smear.put(2 * pair + group, core, refs[2 * pair].at[group])
            smear.put(2 * pair + group, 1 - core, refs[2 * pair + 1].at[group])
    copy = pltpu.make_async_copy(staged_ref, words_ref, sem)
    copy.start()
    smear.shift_matrices()
    copy.wait()
    smear.run_groups(size - 2, partial_ref, pitch)

    def column_block(index):
        return jnp.concatenate(
            [
                early_ref[pl.ds(pl.multiple_of(index * early_pitch, 8), 2 * width), :],
                partial_ref[pl.ds(pl.multiple_of(index * pitch, 8), (size - 2) * width), :],
            ],
            axis=0,
        )

    def multiply_block(step, carry):
        field = jnp.concatenate([column_block(2 * step), column_block(2 * step + 1)], axis=1)
        field_high, field_low = split(field)
        left_high = high_ref[...]
        value = dot(left_high, field_low) + dot(low_ref[...], field_high)
        value = value + dot(left_high, field_high)
        for n in range(2):
            turned = value[:, n * LANES : (n + 1) * LANES].T
            for r in range(0, rows, LANES):
                part = min(LANES, rows - r)
                start = (r // LANES) * (LANES * turn_pitch) + 2 * step + n
                turned_ref[pl.ds(start, LANES, stride=turn_pitch), :part] = turned[:, r : r + part]
        return carry

    lax.fori_loop(0, run // 2, multiply_block, 0)

    per = LANES // run

    def turn_block(step, carry):
        for s in range(slices):
            for r in range(0, rows, LANES):
                part = min(LANES, rows - r)
                base = (r // LANES) * (LANES * turn_pitch)
                pieces = [
                    turned_ref[pl.ds(base + (s * lane_blocks + step * per + n) * turn_pitch, run), :part]
                    for n in range(per)
                ]
                columns = pl.ds(pl.multiple_of(step * LANES, LANES), LANES)
                out_ref[s, r : r + part, columns] = jnp.concatenate(pieces, axis=0).T
        return carry

    lax.fori_loop(0, lane_blocks // per, turn_block, 0)


def body(sinogram, ray_offsets, merge_matrices):
    slices, angles, bin_count = sinogram.shape
    rows = ray_offsets.shape[1]
    margin = rows // SUBLANES
    width = rows // 2 + margin
    size = lax.axis_size("ang")
    tiles = lax.axis_size("tile")
    core = lax.axis_index("tile") & 1
    own_index = lax.axis_index("ang")
    top_bit = jnp.right_shift(own_index, size.bit_length() - 2) & 1
    band_block = top_bit * (SUBLANES // 2 - 1)
    run = slices * bin_count // LANES
    lane_blocks = LANES // slices

    def other_core(array):
        return lax.ppermute(array, "tile", [(i, i ^ 1) for i in range(tiles)])

    def from_group(array, k):
        return lax.ppermute(array, "ang", [(i, i ^ k) for i in range(size)])

    own = packed_rows(sinogram, ray_offsets)
    neighbour = from_group(own, 1)
    mine = jnp.stack([own[core], neighbour[core]])
    place = jnp.stack([core, band_block, own_index]).astype(jnp.int32)

    def spread(count):
        return count + (8 - count) % 32

    early_pitch = spread(2 * width)
    pitch = spread((size - 2) * width)
    turn_pitch = run + 1
    in_vmem = pl.BlockSpec(memory_space=pltpu.VMEM)
    in_smem = pl.BlockSpec(memory_space=pltpu.SMEM)
    smear_sizes = (angles // 2, slices, run, margin, width // margin)

    def smear_scratch(count):
        return [
            pltpu.VMEM((count * angles * run, 2 * LANES), jnp.bfloat16),
            pltpu.VMEM((count * 2 * SUBLANES, LANES), jnp.int32),
            pltpu.SMEM((count * 2 * SUBLANES, LANES), jnp.int32),
            pltpu.VMEM((2 * LANES, lane_blocks * LANES), jnp.bfloat16),
            pltpu.VMEM((angles * (lane_blocks + 1) * run, LANES), jnp.float32),
            pltpu.VMEM((angles * (lane_blocks + 1) * run, LANES), jnp.float32),
        ]

    levels = merge_matrices.shape[0]
    high, low = pl.pallas_call(
        functools.partial(matrices_kernel, levels, width, angles),
        name="matrices",
        out_shape=(jax.ShapeDtypeStruct((rows, size * width), jnp.bfloat16),) * 2,
        in_specs=[in_smem, pl.BlockSpec(memory_space=pl.ANY)],
        out_specs=(in_vmem,) * 2,
        scratch_shapes=[
            pltpu.VMEM((levels,) + merge_matrices.shape[2:], jnp.float32),
            pltpu.SemaphoreType.DMA((levels,)),
        ],
        cost_estimate=pl.CostEstimate(flops=5 * 10**8, bytes_accessed=10**6, transcendentals=0),
        compiler_params=pltpu.CompilerParams(vmem_limit_bytes=32 * 2**20),
    )(place, merge_matrices)
    early = pl.pallas_call(
        functools.partial(early_kernel, smear_sizes, early_pitch),
        name="early",
        out_shape=jax.ShapeDtypeStruct((run * early_pitch, LANES), jnp.float32),
        in_specs=[in_smem] + [in_vmem] * 2,
        out_specs=in_vmem,
        scratch_shapes=smear_scratch(2) + [pltpu.SemaphoreType.DMA],
        cost_estimate=pl.CostEstimate(flops=2 * 10**9, bytes_accessed=10**7, transcendentals=0),
        compiler_params=pltpu.CompilerParams(vmem_limit_bytes=36 * 2**20),
    )(place, own, neighbour)
    mine, high = lax.optimization_barrier((mine, high))
    arrived = [from_group(mine, 2 * pair) for pair in range(1, size // 2)]
    arrived[-1], early = lax.optimization_barrier((arrived[-1], early))
    operands = []
    for array in arrived:
        operands += [array, other_core(array)]
    return pl.pallas_call(
        functools.partial(image_kernel, smear_sizes, size, width, early_pitch, pitch, turn_pitch),
        name="image",
        out_shape=jax.ShapeDtypeStruct((slices, rows, bin_count), jnp.float32),
        in_specs=[in_smem] + [in_vmem] * (size - 2) + [in_vmem] * 3,
        out_specs=in_vmem,
        scratch_shapes=smear_scratch(size - 2)
        + [
            pltpu.VMEM((run * pitch, LANES), jnp.float32),
            pltpu.VMEM((-(-rows // LANES) * LANES * turn_pitch, LANES), jnp.float32),
            pltpu.SemaphoreType.DMA,
        ],
        cost_estimate=pl.CostEstimate(flops=10**10, bytes_accessed=10**7, transcendentals=0),
        compiler_params=pltpu.CompilerParams(vmem_limit_bytes=52 * 2**20),
    )(place, *operands, early, high, low)


def solution(mesh):
    placed = (P(None, "ang", None), P("ang", None), P())
    return jax.shard_map(
        body, mesh=mesh, in_specs=placed, out_specs=P(None, "ang", None), check_vma=False
    )
```

```python
import functools
import math

import jax
import jax.numpy as jnp
from jax import lax
from jax.experimental import pallas as pl
from jax.experimental.pallas import tpu as pltpu
from jax.sharding import PartitionSpec as P

LANES = 128
SUBLANES = 8


def packed_rows(sinogram, ray_offsets):
    slices, angles, bin_count = sinogram.shape
    rows = ray_offsets.shape[1]
    half = angles // 2
    run = slices * bin_count // LANES
    fields = sinogram.reshape(slices, 2, half, bin_count // run, run).transpose(1, 2, 4, 0, 3)
    fields = fields.reshape(2, half * run, LANES)
    words = ray_offsets.astype(jnp.float32).reshape(2, half, SUBLANES, rows // SUBLANES)
    words = words.transpose(0, 2, 1, 3).reshape(2, SUBLANES, -1)
    words = jnp.pad(words, ((0, 0), (0, 0), (0, LANES - words.shape[2])))
    return jnp.concatenate([fields, words], axis=1)


def split(value):
    high = value.astype(jnp.bfloat16)
    return high, (value - high.astype(jnp.float32)).astype(jnp.bfloat16)


def dot(left, right):
    return jnp.dot(left, right, preferred_element_type=jnp.float32)


class Smear:
    def __init__(self, half, slices, run, unroll, core, band, band_blocks, lines, staged, words, shift, tables):
        self.half, self.slices, self.run, self.unroll = half, slices, run, unroll
        self.band, self.band_blocks = band, band_blocks
        self.skip_rows = core * (run // 2)
        self.lines, self.staged, self.words, self.shift, self.tables = lines, staged, words, shift, tables
        self.lane_blocks = LANES // slices
        self.table_rows = (self.lane_blocks + 1) * run
        self.angles = 2 * half

    def put(self, place, part, source):
        size = self.half * self.run
        high, low = split(source[:size, :])
        where = pl.ds(pl.multiple_of((place * 2 + part) * size, size), size)
        self.lines[where, :LANES] = high
        self.lines[where, LANES:] = low
        where = pl.multiple_of((place * 2 + part) * SUBLANES, SUBLANES)
        self.staged[pl.ds(where, SUBLANES), :] = source[size:, :].astype(jnp.int32) + self.skip_rows

    def shift_matrices(self):
        line = lax.broadcasted_iota(jnp.int32, (2 * LANES, LANES), 0)
        lane = lax.broadcasted_iota(jnp.int32, (2 * LANES, LANES), 1)
        same = ((line // self.lane_blocks) % self.slices) == lane // self.lane_blocks
        distance = jnp.where(same, (line - lane) & (self.lane_blocks - 1), -1)
        for m in range(self.lane_blocks):
            self.shift[:, m * LANES : (m + 1) * LANES] = jnp.where(distance == m, 1.0, 0.0).astype(jnp.bfloat16)

    def build(self, place, table, first, count):
        size = self.angles * self.run
        lines = self.lines[place * size : (place + 1) * size, :]
        for m in range(count):
            columns = pl.ds(pl.multiple_of((first + m) * (2 * LANES), 2 * LANES), 2 * LANES)
            shifted = dot(lines, self.shift[:, columns])
            for a in range(self.angles):
                for n in range(2):
                    block = shifted[a * self.run : (a + 1) * self.run, n * LANES : (n + 1) * LANES]
                    start = pl.multiple_of((first + m) * (2 * self.run), SUBLANES)
                    table[pl.ds(start + (a * self.table_rows + n * self.run), self.run), :] = block

    def close(self, table):
        for a in range(self.angles):
            start = a * self.table_rows
            last = start + self.lane_blocks * self.run
            table[last : last + self.run, :] = table[start : start + self.run, :]

    def gather(self, place, table, step, partial, pitch, first, last, skip):
        word_row = place * (2 * SUBLANES) + self.band + step
        first_sample = ((place + skip) * self.band_blocks + step) * self.unroll
        vectors = self.run // (2 * SUBLANES)
        for u in range(first, last):
            sums = [None] * vectors
            for a in range(self.angles):
                offset = self.words[word_row + (a // self.half) * SUBLANES, (a % self.half) * self.unroll + u]
                for n in range(vectors):
                    piece = table[pl.ds(offset + (a * self.table_rows + n * SUBLANES), SUBLANES), :]
                    sums[n] = piece if sums[n] is None else sums[n] + piece
            for n in range(vectors):
                start = first_sample + (u + n * SUBLANES * pitch)
                partial[pl.ds(start, SUBLANES, stride=pitch), :] = sums[n]

    def run_groups(self, count, partial, pitch, skip=0):
        pairs = self.lane_blocks // 2
        share = -(-pairs // self.band_blocks)

        def first_step(step, carry):
            self.build(0, self.tables, jnp.minimum(step * share, pairs - share), share)
            return carry

        lax.fori_loop(0, self.band_blocks, first_step, 0)
        self.close(self.tables)
        for place in range(count):
            now = later = self.tables

            def merged_step(step, carry):
                self.gather(place, now, step, partial, pitch, 0, self.unroll, skip)
                return carry

            lax.fori_loop(0, self.band_blocks, merged_step, 0)
            if place + 1 < count:
                self.build(place + 1, later, 0, pairs)
                self.close(later)


def matrices_kernel(levels, width, angles, place_ref, all_ref, high_ref, low_ref, pair_ref, sems):
    copies = []
    for level in range(levels):
        own_bit = (place_ref[2] >> (levels - 1 - level)) & 1
        copies.append(pltpu.make_async_copy(all_ref.at[level, own_bit], pair_ref.at[level], sems.at[level]))
        copies[-1].start()
    rows = pair_ref.shape[2]
    scale = 1.0 / math.sqrt(angles)
    product = None
    for level in reversed(range(levels)):
        copies[level].wait()
        pair = [pair_ref[level, n] for n in range(2)]
        if level == 0:
            upper = place_ref[1] > 0
            pair = [jnp.where(upper, m[:, rows - width :], m[:, :width]) * scale for m in pair]
        if product is None:
            product = pair
            continue
        pair = [split(m) for m in pair]
        left = [split(m) for m in product]
        product = [
            dot(high, other_low) + dot(low, other_high) + dot(high, other_high)
            for other_high, other_low in pair
            for high, low in left
        ]
    high_ref[...], low_ref[...] = split(jnp.concatenate(product, axis=1))


def early_kernel(smear_sizes, pitch, place_ref, own_ref, neighbour_ref,
                 early_ref, lines_ref, staged_ref, words_ref, shift_ref, table_a, sem):
    half, slices, run, unroll, band_blocks = smear_sizes
    smear = Smear(half, slices, run, unroll, place_ref[0], place_ref[1], band_blocks, lines_ref, staged_ref, words_ref, shift_ref, table_a)
    for part in range(2):
        smear.put(0, part, own_ref.at[part])
        smear.put(1, part, neighbour_ref.at[part])
    copy = pltpu.make_async_copy(staged_ref, words_ref, sem)
    copy.start()
    smear.shift_matrices()
    copy.wait()
    smear.run_groups(2, early_ref, pitch)


def image_kernel(smear_sizes, size, width, early_pitch, pitch, turn_pitch, place_ref, *refs):
    early_ref, high_ref, low_ref = refs[size - 2 : size + 1]
    (out_ref, lines_ref, staged_ref, words_ref, shift_ref, table_a, partial_ref, sem) = refs[size + 1 :]
    half, slices, run, unroll, band_blocks = smear_sizes
    core = place_ref[0]
    smear = Smear(half, slices, run, unroll, place_ref[0], place_ref[1], band_blocks, lines_ref, staged_ref, words_ref, shift_ref, table_a)
    rows = high_ref.shape[0]
    for pair in range(size // 2 - 1):
        for group in range(2):
            smear.put(2 * pair + group, core, refs[2 * pair].at[group])
            smear.put(2 * pair + group, 1 - core, refs[2 * pair + 1].at[group])
    copy = pltpu.make_async_copy(staged_ref, words_ref, sem)
    copy.start()
    smear.shift_matrices()
    copy.wait()
    def copy_early(index, carry):
        where = pl.ds(pl.multiple_of(index * pitch, 8), 2 * width)
        partial_ref[where, :] = early_ref[pl.ds(pl.multiple_of(index * early_pitch, 8), 2 * width), :]
        return carry

    lax.fori_loop(0, run // 2, copy_early, 0)
    smear.run_groups(size - 2, partial_ref, pitch, 2)

    def column_block(index):
        return partial_ref[pl.ds(pl.multiple_of(index * pitch, 8), size * width), :]

    def multiply_block(step, carry):
        field = jnp.concatenate([column_block(2 * step), column_block(2 * step + 1)], axis=1)
        field_high, field_low = split(field)
        left_high = high_ref[...]
        value = dot(left_high, field_low) + dot(low_ref[...], field_high)
        value = value + dot(left_high, field_high)
        for n in range(2):
            turned = value[:, n * LANES : (n + 1) * LANES].T
            for r in range(0, rows, LANES):
                part = min(LANES, rows - r)
                start = (r // LANES) * (LANES * turn_pitch) + 2 * step + n
                out_ref[pl.ds(start, LANES, stride=turn_pitch), :part] = turned[:, r : r + part]
        return carry

    lax.fori_loop(0, run // 4, multiply_block, 0, unroll=2)


def finish_kernel(slices, run, turn_pitch, place_ref, own_ref, other_ref, out_ref):
    swap = place_ref[0] == 0
    lane_blocks = LANES // slices
    per = LANES // run
    part = out_ref.shape[1]

    def turn_block(step, carry):
        for s in range(slices):
            pieces = []
            for n in range(per):
                rows = pl.ds((s * lane_blocks + step * per + n) * turn_pitch, run // 2)
                own, other = own_ref[rows, :], other_ref[rows, :]
                pieces += [jnp.where(swap, own, other), jnp.where(swap, other, own)]
            columns = pl.ds(pl.multiple_of(step * LANES, LANES), LANES)
            out_ref[s, :, columns] = jnp.concatenate(pieces, axis=0).T[:part]
        return carry

    lax.fori_loop(0, lane_blocks // per, turn_block, 0, unroll=2)


def body(sinogram, ray_offsets, merge_matrices):
    slices, angles, bin_count = sinogram.shape
    rows = ray_offsets.shape[1]
    margin = rows // SUBLANES
    width = rows // 2 + margin
    size = lax.axis_size("ang")
    tiles = lax.axis_size("tile")
    core = lax.axis_index("tile") & 1
    own_index = lax.axis_index("ang")
    top_bit = jnp.right_shift(own_index, size.bit_length() - 2) & 1
    band_block = top_bit * (SUBLANES // 2 - 1)
    run = slices * bin_count // LANES
    lane_blocks = LANES // slices

    def other_core(array):
        return lax.ppermute(array, "tile", [(i, i ^ 1) for i in range(tiles)])

    def from_group(array, k):
        return lax.ppermute(array, "ang", [(i, i ^ k) for i in range(size)])

    own = packed_rows(sinogram, ray_offsets)
    neighbour = from_group(own, 1)
    mine = jnp.stack([own[core], neighbour[core]])
    place = jnp.stack([core, band_block, own_index]).astype(jnp.int32)

    def spread(count):
        return count + (8 - count) % 32

    early_pitch = spread(2 * width)
    pitch = spread(size * width)
    turn_pitch = run // 2 + 1
    turn_blocks = -(-rows // LANES)
    turned_rows = LANES * turn_pitch
    in_vmem = pl.BlockSpec(memory_space=pltpu.VMEM)
    in_smem = pl.BlockSpec(memory_space=pltpu.SMEM)
    smear_sizes = (angles // 2, slices, run, margin, width // margin)

    def smear_scratch(count):
        return [
            pltpu.VMEM((count * angles * run, 2 * LANES), jnp.bfloat16),
            pltpu.VMEM((count * 2 * SUBLANES, LANES), jnp.int32),
            pltpu.SMEM((count * 2 * SUBLANES, LANES), jnp.int32),
            pltpu.VMEM((2 * LANES, lane_blocks * LANES), jnp.bfloat16),
            pltpu.VMEM((angles * (lane_blocks + 1) * run, LANES), jnp.float32),
        ]

    levels = merge_matrices.shape[0]
    high, low = pl.pallas_call(
        functools.partial(matrices_kernel, levels, width, angles),
        name="matrices",
        out_shape=(jax.ShapeDtypeStruct((rows, size * width), jnp.bfloat16),) * 2,
        in_specs=[in_smem, pl.BlockSpec(memory_space=pltpu.HBM)],
        out_specs=(in_vmem,) * 2,
        scratch_shapes=[
            pltpu.VMEM((levels,) + merge_matrices.shape[2:], jnp.float32),
            pltpu.SemaphoreType.DMA((levels,)),
        ],
        cost_estimate=pl.CostEstimate(flops=5 * 10**8, bytes_accessed=10**6, transcendentals=0),
        compiler_params=pltpu.CompilerParams(vmem_limit_bytes=32 * 2**20),
    )(place, merge_matrices)
    early = pl.pallas_call(
        functools.partial(early_kernel, smear_sizes, early_pitch),
        name="early",
        out_shape=jax.ShapeDtypeStruct((run // 2 * early_pitch, LANES), jnp.float32),
        in_specs=[in_smem] + [in_vmem] * 2,
        out_specs=in_vmem,
        scratch_shapes=smear_scratch(2) + [pltpu.SemaphoreType.DMA],
        cost_estimate=pl.CostEstimate(flops=2 * 10**9, bytes_accessed=10**7, transcendentals=0),
        compiler_params=pltpu.CompilerParams(vmem_limit_bytes=36 * 2**20),
    )(place, own, neighbour)
    mine, high = lax.optimization_barrier((mine, high))
    arrived = [from_group(mine, 2 * pair) for pair in range(1, size // 2)]
    arrived[-1], early = lax.optimization_barrier((arrived[-1], early))
    operands = []
    for array in arrived:
        operands += [array, other_core(array)]
    turned = pl.pallas_call(
        functools.partial(image_kernel, smear_sizes, size, width, early_pitch, pitch, turn_pitch),
        name="image",
        out_shape=jax.ShapeDtypeStruct((turn_blocks * turned_rows, LANES), jnp.float32),
        in_specs=[in_smem] + [in_vmem] * (size - 2) + [in_vmem] * 3,
        out_specs=in_vmem,
        scratch_shapes=smear_scratch(size - 2)
        + [
            pltpu.VMEM((run // 2 * pitch, LANES), jnp.float32),
            pltpu.SemaphoreType.DMA,
        ],
        cost_estimate=pl.CostEstimate(flops=10**10, bytes_accessed=10**7, transcendentals=0),
        compiler_params=pltpu.CompilerParams(vmem_limit_bytes=40 * 2**20),
    )(place, *operands, early, high, low)
    rows_spec = pl.BlockSpec((turned_rows, LANES), lambda i: (i, 0))
    block_rows = min(rows, LANES)
    return pl.pallas_call(
        functools.partial(finish_kernel, slices, run, turn_pitch),
        name="finish",
        out_shape=jax.ShapeDtypeStruct((slices, rows, bin_count), jnp.float32),
        grid=(turn_blocks,),
        in_specs=[in_smem, rows_spec, rows_spec],
        out_specs=pl.BlockSpec((slices, block_rows, bin_count), lambda i: (0, i, 0)),
        cost_estimate=pl.CostEstimate(flops=10**8, bytes_accessed=10**7, transcendentals=0),
        compiler_params=pltpu.CompilerParams(vmem_limit_bytes=24 * 2**20),
    )(place, turned, other_core(turned))


def solution(mesh):
    placed = (P(None, "ang", None), P("ang", None), P())
    return jax.shard_map(
        body, mesh=mesh, in_specs=placed, out_specs=P(None, "ang", None), check_vma=False
    )
```

```python
import functools
import math

import jax
import jax.numpy as jnp
from jax import lax
from jax.experimental import pallas as pl
from jax.experimental.pallas import tpu as pltpu
from jax.sharding import PartitionSpec as P

LANES = 128
SUBLANES = 8


def packed_rows(sinogram, ray_offsets):
    slices, angles, bin_count = sinogram.shape
    rows = ray_offsets.shape[1]
    half = angles // 2
    run = slices * bin_count // LANES
    fields = sinogram.reshape(slices, 2, half, bin_count // run, run).transpose(1, 2, 4, 0, 3)
    fields = fields.reshape(2, half * run, LANES)
    words = ray_offsets.astype(jnp.float32).reshape(2, half, SUBLANES, rows // SUBLANES)
    words = words.transpose(0, 2, 1, 3).reshape(2, SUBLANES, -1)
    words = jnp.pad(words, ((0, 0), (0, 0), (0, LANES - words.shape[2])))
    return jnp.concatenate([fields, words], axis=1)


def split(value):
    high = value.astype(jnp.bfloat16)
    return high, (value - high.astype(jnp.float32)).astype(jnp.bfloat16)


def dot(left, right):
    return jnp.dot(left, right, preferred_element_type=jnp.float32)


class Smear:
    def __init__(self, half, slices, run, unroll, core, band, band_blocks, lines, staged, words, shift, tables):
        self.half, self.slices, self.run, self.unroll = half, slices, run, unroll
        self.band, self.band_blocks = band, band_blocks
        self.skip_rows = core * (run // 2)
        self.lines, self.staged, self.words, self.shift, self.tables = lines, staged, words, shift, tables
        self.lane_blocks = LANES // slices
        self.table_rows = (self.lane_blocks + 1) * run
        self.angles = 2 * half

    def put(self, place, part, source):
        size = self.half * self.run
        high, low = split(source[:size, :])
        where = pl.ds(pl.multiple_of((place * 2 + part) * size, size), size)
        self.lines[where, :LANES] = high
        self.lines[where, LANES:] = low
        where = pl.multiple_of((place * 2 + part) * SUBLANES, SUBLANES)
        self.staged[pl.ds(where, SUBLANES), :] = source[size:, :].astype(jnp.int32) + self.skip_rows

    def shift_matrices(self):
        line = lax.broadcasted_iota(jnp.int32, (2 * LANES, LANES), 0)
        lane = lax.broadcasted_iota(jnp.int32, (2 * LANES, LANES), 1)
        same = ((line // self.lane_blocks) % self.slices) == lane // self.lane_blocks
        distance = jnp.where(same, (line - lane) & (self.lane_blocks - 1), -1)
        for m in range(self.lane_blocks):
            self.shift[:, m * LANES : (m + 1) * LANES] = jnp.where(distance == m, 1.0, 0.0).astype(jnp.bfloat16)

    def build(self, place, table, first, count):
        size = self.angles * self.run
        lines = self.lines[place * size : (place + 1) * size, :]
        for m in range(count):
            columns = pl.ds(pl.multiple_of((first + m) * (2 * LANES), 2 * LANES), 2 * LANES)
            shifted = dot(lines, self.shift[:, columns])
            for a in range(self.angles):
                for n in range(2):
                    block = shifted[a * self.run : (a + 1) * self.run, n * LANES : (n + 1) * LANES]
                    start = pl.multiple_of((first + m) * (2 * self.run), SUBLANES)
                    table[pl.ds(start + (a * self.table_rows + n * self.run), self.run), :] = block

    def close(self, table):
        for a in range(self.angles):
            start = a * self.table_rows
            last = start + self.lane_blocks * self.run
            table[last : last + self.run, :] = table[start : start + self.run, :]

    def gather(self, place, table, step, partial, pitch, first, last, skip):
        word_row = place * (2 * SUBLANES) + self.band + step
        first_sample = ((place + skip) * self.band_blocks + step) * self.unroll
        vectors = self.run // (2 * SUBLANES)
        for u in range(first, last):
            sums = [None] * vectors
            for a in range(self.angles):
                offset = self.words[word_row + (a // self.half) * SUBLANES, (a % self.half) * self.unroll + u]
                for n in range(vectors):
                    piece = table[pl.ds(offset + (a * self.table_rows + n * SUBLANES), SUBLANES), :]
                    sums[n] = piece if sums[n] is None else sums[n] + piece
            for n in range(vectors):
                start = first_sample + (u + n * SUBLANES * pitch)
                partial[pl.ds(start, SUBLANES, stride=pitch), :] = sums[n]

    def run_groups(self, count, partial, pitch, skip=0):
        pairs = self.lane_blocks // 2
        self.build(0, self.tables, 0, pairs)
        self.close(self.tables)
        for place in range(count):
            now = later = self.tables

            def merged_step(step, carry):
                self.gather(place, now, step, partial, pitch, 0, self.unroll, skip)
                return carry

            lax.fori_loop(0, self.band_blocks, merged_step, 0)
            if place + 1 < count:
                self.build(place + 1, later, 0, pairs)
                self.close(later)


def matrices_kernel(levels, width, angles, place_ref, all_ref, high_ref, low_ref, pair_ref, sems):
    copies = []
    for level in range(levels):
        own_bit = (place_ref[2] >> (levels - 1 - level)) & 1
        copies.append(pltpu.make_async_copy(all_ref.at[level, own_bit], pair_ref.at[level], sems.at[level]))
        copies[-1].start()
    rows = pair_ref.shape[2]
    scale = 1.0 / math.sqrt(angles)
    product = None
    for level in reversed(range(levels)):
        copies[level].wait()
        pair = [pair_ref[level, n] for n in range(2)]
        if level == 0:
            upper = place_ref[1] > 0
            pair = [jnp.where(upper, m[:, rows - width :], m[:, :width]) * scale for m in pair]
        if product is None:
            product = pair
            continue
        pair = [split(m) for m in pair]
        left = [split(m) for m in product]
        product = [
            dot(high, other_low) + dot(low, other_high) + dot(high, other_high)
            for other_high, other_low in pair
            for high, low in left
        ]
    high_ref[...], low_ref[...] = split(jnp.concatenate(product, axis=1))


def early_kernel(smear_sizes, pitch, place_ref, own_ref, neighbour_ref,
                 early_ref, shift_ref, lines_ref, staged_ref, words_ref, table_a, sem):
    half, slices, run, unroll, band_blocks = smear_sizes
    smear = Smear(half, slices, run, unroll, place_ref[0], place_ref[1], band_blocks, lines_ref, staged_ref, words_ref, shift_ref, table_a)
    for part in range(2):
        smear.put(0, part, own_ref.at[part])
        smear.put(1, part, neighbour_ref.at[part])
    copy = pltpu.make_async_copy(staged_ref, words_ref, sem)
    copy.start()
    smear.shift_matrices()
    copy.wait()
    smear.run_groups(2, early_ref, pitch)


def image_kernel(smear_sizes, size, width, early_pitch, pitch, turn_pitch, place_ref, *refs):
    early_ref, shift_ref, high_ref, low_ref = refs[size - 2 : size + 2]
    (out_ref, lines_ref, staged_ref, words_ref, table_a, partial_ref, sem) = refs[size + 2 :]
    half, slices, run, unroll, band_blocks = smear_sizes
    core = place_ref[0]
    smear = Smear(half, slices, run, unroll, place_ref[0], place_ref[1], band_blocks, lines_ref, staged_ref, words_ref, shift_ref, table_a)
    rows = high_ref.shape[0]
    for pair in range(size // 2 - 1):
        for group in range(2):
            smear.put(2 * pair + group, core, refs[2 * pair].at[group])
            smear.put(2 * pair + group, 1 - core, refs[2 * pair + 1].at[group])
    copy = pltpu.make_async_copy(staged_ref, words_ref, sem)
    copy.start()
    copy.wait()
    def copy_early(index, carry):
        where = pl.ds(index * pitch, 2 * width)
        partial_ref[where, :] = early_ref[pl.ds(index * early_pitch, 2 * width), :]
        return carry

    lax.fori_loop(0, run // 2, copy_early, 0)
    smear.run_groups(size - 2, partial_ref, pitch, 2)

    def column_block(index):
        return partial_ref[pl.ds(index * pitch, size * width), :]

    def multiply_block(step, carry):
        field = jnp.concatenate([column_block(2 * step), column_block(2 * step + 1)], axis=1)
        field_high, field_low = split(field)
        left_high = high_ref[...]
        value = dot(left_high, field_low) + dot(low_ref[...], field_high)
        value = value + dot(left_high, field_high)
        for n in range(2):
            turned = value[:, n * LANES : (n + 1) * LANES].T
            for r in range(0, rows, LANES):
                part = min(LANES, rows - r)
                start = (r // LANES) * (LANES * turn_pitch) + 2 * step + n
                out_ref[pl.ds(start, LANES, stride=turn_pitch), :part] = turned[:, r : r + part]
        return carry

    lax.fori_loop(0, run // 4, multiply_block, 0, unroll=4)


def finish_kernel(slices, run, turn_pitch, place_ref, own_ref, other_ref, out_ref):
    swap = place_ref[0] == 0
    lane_blocks = LANES // slices
    per = LANES // run
    part = out_ref.shape[1]

    def turn_block(step, carry):
        for s in range(slices):
            pieces = []
            for n in range(per):
                rows = pl.ds((s * lane_blocks + step * per + n) * turn_pitch, run // 2)
                own, other = own_ref[rows, :], other_ref[rows, :]
                pieces += [jnp.where(swap, own, other), jnp.where(swap, other, own)]
            columns = pl.ds(pl.multiple_of(step * LANES, LANES), LANES)
            out_ref[s, :, columns] = jnp.concatenate(pieces, axis=0).T[:part]
        return carry

    lax.fori_loop(0, lane_blocks // per, turn_block, 0, unroll=4)


def body(sinogram, ray_offsets, merge_matrices):
    slices, angles, bin_count = sinogram.shape
    rows = ray_offsets.shape[1]
    margin = rows // SUBLANES
    width = rows // 2 + margin
    size = lax.axis_size("ang")
    tiles = lax.axis_size("tile")
    core = lax.axis_index("tile") & 1
    own_index = lax.axis_index("ang")
    top_bit = jnp.right_shift(own_index, size.bit_length() - 2) & 1
    band_block = top_bit * (SUBLANES // 2 - 1)
    run = slices * bin_count // LANES
    lane_blocks = LANES // slices

    def other_core(array):
        return lax.ppermute(array, "tile", [(i, i ^ 1) for i in range(tiles)])

    def from_group(array, k):
        return lax.ppermute(array, "ang", [(i, i ^ k) for i in range(size)])

    own = packed_rows(sinogram, ray_offsets)
    neighbour = from_group(own, 1)
    mine = jnp.stack([own[core], neighbour[core]])
    place = jnp.stack([core, band_block, own_index]).astype(jnp.int32)

    def spread(count):
        return count + (12 - count) % 32

    early_pitch = spread(2 * width)
    pitch = spread(size * width)
    turn_pitch = run // 2 + 1
    turn_blocks = -(-rows // LANES)
    turned_rows = LANES * turn_pitch
    in_vmem = pl.BlockSpec(memory_space=pltpu.VMEM)
    in_smem = pl.BlockSpec(memory_space=pltpu.SMEM)
    smear_sizes = (angles // 2, slices, run, margin, width // margin)

    def smear_scratch(count):
        return [
            pltpu.VMEM((count * angles * run, 2 * LANES), jnp.bfloat16),
            pltpu.VMEM((count * 2 * SUBLANES, LANES), jnp.int32),
            pltpu.SMEM((count * 2 * SUBLANES, LANES), jnp.int32),
            pltpu.VMEM((angles * (lane_blocks + 1) * run, LANES), jnp.float32),
        ]

    levels = merge_matrices.shape[0]
    high, low = pl.pallas_call(
        functools.partial(matrices_kernel, levels, width, angles),
        name="matrices",
        out_shape=(jax.ShapeDtypeStruct((rows, size * width), jnp.bfloat16),) * 2,
        in_specs=[in_smem, pl.BlockSpec(memory_space=pltpu.HBM)],
        out_specs=(in_vmem,) * 2,
        scratch_shapes=[
            pltpu.VMEM((levels,) + merge_matrices.shape[2:], jnp.float32),
            pltpu.SemaphoreType.DMA((levels,)),
        ],
        cost_estimate=pl.CostEstimate(flops=5 * 10**8, bytes_accessed=10**6, transcendentals=0),
        compiler_params=pltpu.CompilerParams(vmem_limit_bytes=32 * 2**20),
    )(place, merge_matrices)
    early, shift = pl.pallas_call(
        functools.partial(early_kernel, smear_sizes, early_pitch),
        name="early",
        out_shape=(
            jax.ShapeDtypeStruct((run // 2 * early_pitch, LANES), jnp.float32),
            jax.ShapeDtypeStruct((2 * LANES, lane_blocks * LANES), jnp.bfloat16),
        ),
        in_specs=[in_smem] + [in_vmem] * 2,
        out_specs=(in_vmem,) * 2,
        scratch_shapes=smear_scratch(2) + [pltpu.SemaphoreType.DMA],
        cost_estimate=pl.CostEstimate(flops=2 * 10**9, bytes_accessed=10**7, transcendentals=0),
        compiler_params=pltpu.CompilerParams(vmem_limit_bytes=28 * 2**20),
    )(place, own, neighbour)
    arrived = [from_group(mine, 2 * pair) for pair in range(1, size // 2)]
    arrived[-1], early, high = lax.optimization_barrier((arrived[-1], early, high))
    operands = []
    for array in arrived:
        operands += [array, other_core(array)]
    turned = pl.pallas_call(
        functools.partial(image_kernel, smear_sizes, size, width, early_pitch, pitch, turn_pitch),
        name="image",
        out_shape=jax.ShapeDtypeStruct((turn_blocks * turned_rows, LANES), jnp.float32),
        in_specs=[in_smem] + [in_vmem] * (size - 2) + [in_vmem] * 4,
        out_specs=in_vmem,
        scratch_shapes=smear_scratch(size - 2)
        + [
            pltpu.VMEM((run // 2 * pitch, LANES), jnp.float32),
            pltpu.SemaphoreType.DMA,
        ],
        cost_estimate=pl.CostEstimate(flops=10**10, bytes_accessed=10**7, transcendentals=0),
        compiler_params=pltpu.CompilerParams(vmem_limit_bytes=30 * 2**20),
    )(place, *operands, early, shift, high, low)
    rows_spec = pl.BlockSpec((turned_rows, LANES), lambda i: (i, 0))
    block_rows = min(rows, LANES)
    return pl.pallas_call(
        functools.partial(finish_kernel, slices, run, turn_pitch),
        name="finish",
        out_shape=jax.ShapeDtypeStruct((slices, rows, bin_count), jnp.float32),
        grid=(turn_blocks,),
        in_specs=[in_smem, rows_spec, rows_spec],
        out_specs=pl.BlockSpec((slices, block_rows, bin_count), lambda i: (0, i, 0)),
        cost_estimate=pl.CostEstimate(flops=10**8, bytes_accessed=10**7, transcendentals=0),
        compiler_params=pltpu.CompilerParams(vmem_limit_bytes=24 * 2**20),
    )(place, turned, other_core(turned))


def solution(mesh):
    placed = (P(None, "ang", None), P("ang", None), P())
    return jax.shard_map(
        body, mesh=mesh, in_specs=placed, out_specs=P(None, "ang", None), check_vma=False
    )
```

```python
import functools
import math

import jax
import jax.numpy as jnp
from jax import lax
from jax.experimental import pallas as pl
from jax.experimental.pallas import tpu as pltpu
from jax.sharding import PartitionSpec as P

LANES = 128
SUBLANES = 8


def packed_rows(sinogram, ray_offsets):
    slices, angles, bin_count = sinogram.shape
    rows = ray_offsets.shape[1]
    half = angles // 2
    run = slices * bin_count // LANES
    fields = sinogram.reshape(slices, 2, half, bin_count // run, run).transpose(1, 2, 4, 0, 3)
    fields = fields.reshape(2, half * run, LANES)
    words = ray_offsets.astype(jnp.float32).reshape(2, half, SUBLANES, rows // SUBLANES)
    words = words.transpose(0, 2, 1, 3).reshape(2, SUBLANES, -1)
    words = jnp.pad(words, ((0, 0), (0, 0), (0, LANES - words.shape[2])))
    return jnp.concatenate([fields, words], axis=1)


def split(value):
    high = value.astype(jnp.bfloat16)
    return high, (value - high.astype(jnp.float32)).astype(jnp.bfloat16)


def dot(left, right):
    return jnp.dot(left, right, preferred_element_type=jnp.float32)


class Smear:
    def __init__(self, half, slices, run, unroll, core, band, band_blocks, lines, staged, words, shift, tables):
        self.half, self.slices, self.run, self.unroll = half, slices, run, unroll
        self.band, self.band_blocks = band, band_blocks
        self.skip_rows = core * (run // 2)
        self.lines, self.staged, self.words, self.shift, self.tables = lines, staged, words, shift, tables
        self.lane_blocks = LANES // slices
        self.table_rows = (self.lane_blocks + 1) * run
        self.angles = 2 * half

    def put(self, place, part, source):
        size = self.half * self.run
        high, low = split(source[:size, :])
        where = pl.ds(pl.multiple_of((place * 2 + part) * size, size), size)
        self.lines[where, :LANES] = high
        self.lines[where, LANES:] = low
        where = pl.multiple_of((place * 2 + part) * SUBLANES, SUBLANES)
        self.staged[pl.ds(where, SUBLANES), :] = source[size:, :].astype(jnp.int32) + self.skip_rows

    def shift_matrices(self):
        line = lax.broadcasted_iota(jnp.int32, (2 * LANES, LANES), 0)
        lane = lax.broadcasted_iota(jnp.int32, (2 * LANES, LANES), 1)
        same = ((line // self.lane_blocks) % self.slices) == lane // self.lane_blocks
        distance = jnp.where(same, (line - lane) & (self.lane_blocks - 1), -1)
        for m in range(self.lane_blocks):
            self.shift[:, m * LANES : (m + 1) * LANES] = jnp.where(distance == m, 1.0, 0.0).astype(jnp.bfloat16)

    def build(self, place, table, first, count):
        size = self.angles * self.run
        lines = self.lines[place * size : (place + 1) * size, :]
        for m in range(count):
            columns = pl.ds(pl.multiple_of((first + m) * (2 * LANES), 2 * LANES), 2 * LANES)
            shifted = dot(lines, self.shift[:, columns])
            for a in range(self.angles):
                for n in range(2):
                    block = shifted[a * self.run : (a + 1) * self.run, n * LANES : (n + 1) * LANES]
                    start = pl.multiple_of((first + m) * (2 * self.run), SUBLANES)
                    table[pl.ds(start + (a * self.table_rows + n * self.run), self.run), :] = block

    def close(self, table):
        for a in range(self.angles):
            start = a * self.table_rows
            last = start + self.lane_blocks * self.run
            table[last : last + self.run, :] = table[start : start + self.run, :]

    def gather(self, place, table, step, partial, pitch, first, last, skip):
        word_row = place * (2 * SUBLANES) + self.band + step
        first_sample = ((place + skip) * self.band_blocks + step) * self.unroll
        vectors = self.run // (2 * SUBLANES)
        for u in range(first, last):
            sums = [None] * vectors
            for a in range(self.angles):
                offset = self.words[word_row + (a // self.half) * SUBLANES, (a % self.half) * self.unroll + u]
                for n in range(vectors):
                    piece = table[pl.ds(offset + (a * self.table_rows + n * SUBLANES), SUBLANES), :]
                    sums[n] = piece if sums[n] is None else sums[n] + piece
            for n in range(vectors):
                start = first_sample + (u + n * SUBLANES * pitch)
                partial[pl.ds(start, SUBLANES, stride=pitch), :] = sums[n]

    def run_groups(self, count, partial, pitch, skip=0):
        pairs = self.lane_blocks // 2
        self.build(0, self.tables, 0, pairs)
        self.close(self.tables)
        for place in range(count):
            now = later = self.tables

            def merged_step(step, carry):
                self.gather(place, now, step, partial, pitch, 0, self.unroll, skip)
                return carry

            lax.fori_loop(0, self.band_blocks, merged_step, 0)
            if place + 1 < count:
                self.build(place + 1, later, 0, pairs)
                self.close(later)


def matrices_kernel(levels, width, angles, place_ref, all_ref, high_ref, low_ref, pair_ref, sems):
    copies = []
    for level in range(levels):
        own_bit = (place_ref[2] >> (levels - 1 - level)) & 1
        copies.append(pltpu.make_async_copy(all_ref.at[level, own_bit], pair_ref.at[level], sems.at[level]))
        copies[-1].start()
    rows = pair_ref.shape[2]
    scale = 1.0 / math.sqrt(angles)
    product = None
    for level in reversed(range(levels)):
        copies[level].wait()
        pair = [pair_ref[level, n] for n in range(2)]
        if level == 0:
            upper = place_ref[1] > 0
            pair = [jnp.where(upper, m[:, rows - width :], m[:, :width]) * scale for m in pair]
        if product is None:
            product = pair
            continue
        pair = [split(m) for m in pair]
        left = [split(m) for m in product]
        product = [
            dot(high, other_low) + dot(low, other_high) + dot(high, other_high)
            for other_high, other_low in pair
            for high, low in left
        ]
    high_ref[...], low_ref[...] = split(jnp.concatenate(product, axis=1))


def early_kernel(smear_sizes, pitch, place_ref, own_ref, neighbour_ref,
                 early_ref, shift_ref, lines_ref, staged_ref, words_ref, table_a, sem):
    half, slices, run, unroll, band_blocks = smear_sizes
    smear = Smear(half, slices, run, unroll, place_ref[0], place_ref[1], band_blocks, lines_ref, staged_ref, words_ref, shift_ref, table_a)
    for part in range(2):
        smear.put(0, part, own_ref.at[part])
        smear.put(1, part, neighbour_ref.at[part])
    copy = pltpu.make_async_copy(staged_ref, words_ref, sem)
    copy.start()
    smear.shift_matrices()
    copy.wait()
    smear.run_groups(2, early_ref, pitch)


def image_kernel(smear_sizes, size, width, early_pitch, pitch, turn_pitch, place_ref, *refs):
    early_ref, shift_ref, high_ref, low_ref = refs[size - 2 : size + 2]
    (out_ref, lines_ref, staged_ref, words_ref, table_a, partial_ref, sem) = refs[size + 2 :]
    half, slices, run, unroll, band_blocks = smear_sizes
    core = place_ref[0]
    smear = Smear(half, slices, run, unroll, place_ref[0], place_ref[1], band_blocks, lines_ref, staged_ref, words_ref, shift_ref, table_a)
    rows = high_ref.shape[0]
    for pair in range(size // 2 - 1):
        for group in range(2):
            smear.put(2 * pair + group, core, refs[2 * pair].at[group])
            smear.put(2 * pair + group, 1 - core, refs[2 * pair + 1].at[group])
    copy = pltpu.make_async_copy(staged_ref, words_ref, sem)
    copy.start()
    copy.wait()
    def copy_early(index, carry):
        where = pl.ds(index * pitch, 2 * width)
        partial_ref[where, :] = early_ref[pl.ds(index * early_pitch, 2 * width), :]
        return carry

    lax.fori_loop(0, run // 2, copy_early, 0)
    smear.run_groups(size - 2, partial_ref, pitch, 2)

    def column_block(index):
        return partial_ref[pl.ds(index * pitch, size * width), :]

    def multiply_block(step, carry):
        field = jnp.concatenate([column_block(2 * step), column_block(2 * step + 1)], axis=1)
        field_high, field_low = split(field)
        left_high = high_ref[...]
        value = dot(left_high, field_low) + dot(low_ref[...], field_high)
        value = value + dot(left_high, field_high)
        for n in range(2):
            turned = value[:, n * LANES : (n + 1) * LANES].T
            for r in range(0, rows, LANES):
                part = min(LANES, rows - r)
                start = (r // LANES) * (LANES * turn_pitch) + 2 * step + n
                out_ref[pl.ds(start, LANES, stride=turn_pitch), :part] = turned[:, r : r + part]
        return carry

    lax.fori_loop(0, run // 4, multiply_block, 0, unroll=8)


def finish_kernel(slices, run, turn_pitch, place_ref, own_ref, other_ref, out_ref):
    swap = place_ref[0] == 0
    lane_blocks = LANES // slices
    per = LANES // run
    part = out_ref.shape[1]

    def turn_block(step, carry):
        for s in range(slices):
            pieces = []
            for n in range(per):
                rows = pl.ds((s * lane_blocks + step * per + n) * turn_pitch, run // 2)
                own, other = own_ref[rows, :], other_ref[rows, :]
                pieces += [jnp.where(swap, own, other), jnp.where(swap, other, own)]
            columns = pl.ds(pl.multiple_of(step * LANES, LANES), LANES)
            out_ref[s, :, columns] = jnp.concatenate(pieces, axis=0).T[:part]
        return carry

    lax.fori_loop(0, lane_blocks // per, turn_block, 0, unroll=8)


def body(sinogram, ray_offsets, merge_matrices):
    slices, angles, bin_count = sinogram.shape
    rows = ray_offsets.shape[1]
    margin = rows // SUBLANES
    width = rows // 2 + margin
    size = lax.axis_size("ang")
    tiles = lax.axis_size("tile")
    core = lax.axis_index("tile") & 1
    own_index = lax.axis_index("ang")
    top_bit = jnp.right_shift(own_index, size.bit_length() - 2) & 1
    band_block = top_bit * (SUBLANES // 2 - 1)
    run = slices * bin_count // LANES
    lane_blocks = LANES // slices

    def other_core(array):
        return lax.ppermute(array, "tile", [(i, i ^ 1) for i in range(tiles)])

    def from_group(array, k):
        return lax.ppermute(array, "ang", [(i, i ^ k) for i in range(size)])

    own = packed_rows(sinogram, ray_offsets)
    neighbour = from_group(own, 1)
    mine = jnp.stack([own[core], neighbour[core]])
    place = jnp.stack([core, band_block, own_index]).astype(jnp.int32)

    def spread(count):
        return count + (12 - count) % 32

    early_pitch = spread(2 * width)
    pitch = spread(size * width)
    turn_pitch = run // 2 + 1
    turn_blocks = -(-rows // LANES)
    turned_rows = LANES * turn_pitch
    in_vmem = pl.BlockSpec(memory_space=pltpu.VMEM)
    in_smem = pl.BlockSpec(memory_space=pltpu.SMEM)
    smear_sizes = (angles // 2, slices, run, margin, width // margin)

    def smear_scratch(count):
        return [
            pltpu.VMEM((count * angles * run, 2 * LANES), jnp.bfloat16),
            pltpu.VMEM((count * 2 * SUBLANES, LANES), jnp.int32),
            pltpu.SMEM((count * 2 * SUBLANES, LANES), jnp.int32),
            pltpu.VMEM((angles * (lane_blocks + 1) * run, LANES), jnp.float32),
        ]

    levels = merge_matrices.shape[0]
    high, low = pl.pallas_call(
        functools.partial(matrices_kernel, levels, width, angles),
        name="matrices",
        out_shape=(jax.ShapeDtypeStruct((rows, size * width), jnp.bfloat16),) * 2,
        in_specs=[in_smem, pl.BlockSpec(memory_space=pltpu.HBM)],
        out_specs=(in_vmem,) * 2,
        scratch_shapes=[
            pltpu.VMEM((levels,) + merge_matrices.shape[2:], jnp.float32),
            pltpu.SemaphoreType.DMA((levels,)),
        ],
        cost_estimate=pl.CostEstimate(flops=5 * 10**8, bytes_accessed=10**6, transcendentals=0),
        compiler_params=pltpu.CompilerParams(vmem_limit_bytes=32 * 2**20),
    )(place, merge_matrices)
    early, shift = pl.pallas_call(
        functools.partial(early_kernel, smear_sizes, early_pitch),
        name="early",
        out_shape=(
            jax.ShapeDtypeStruct((run // 2 * early_pitch, LANES), jnp.float32),
            jax.ShapeDtypeStruct((2 * LANES, lane_blocks * LANES), jnp.bfloat16),
        ),
        in_specs=[in_smem] + [in_vmem] * 2,
        out_specs=(in_vmem,) * 2,
        scratch_shapes=smear_scratch(2) + [pltpu.SemaphoreType.DMA],
        cost_estimate=pl.CostEstimate(flops=2 * 10**9, bytes_accessed=10**7, transcendentals=0),
        compiler_params=pltpu.CompilerParams(vmem_limit_bytes=28 * 2**20),
    )(place, own, neighbour)
    arrived = [from_group(mine, 2 * pair) for pair in range(1, size // 2)]
    arrived[-1], early, high = lax.optimization_barrier((arrived[-1], early, high))
    operands = []
    for array in arrived:
        operands += [array, other_core(array)]
    turned = pl.pallas_call(
        functools.partial(image_kernel, smear_sizes, size, width, early_pitch, pitch, turn_pitch),
        name="image",
        out_shape=jax.ShapeDtypeStruct((turn_blocks * turned_rows, LANES), jnp.float32),
        in_specs=[in_smem] + [in_vmem] * (size - 2) + [in_vmem] * 4,
        out_specs=in_vmem,
        scratch_shapes=smear_scratch(size - 2)
        + [
            pltpu.VMEM((run // 2 * pitch, LANES), jnp.float32),
            pltpu.SemaphoreType.DMA,
        ],
        cost_estimate=pl.CostEstimate(flops=10**10, bytes_accessed=10**7, transcendentals=0),
        compiler_params=pltpu.CompilerParams(vmem_limit_bytes=30 * 2**20),
    )(place, *operands, early, shift, high, low)
    rows_spec = pl.BlockSpec((turned_rows, LANES), lambda i: (i, 0))
    block_rows = min(rows, LANES)
    return pl.pallas_call(
        functools.partial(finish_kernel, slices, run, turn_pitch),
        name="finish",
        out_shape=jax.ShapeDtypeStruct((slices, rows, bin_count), jnp.float32),
        grid=(turn_blocks,),
        in_specs=[in_smem, rows_spec, rows_spec],
        out_specs=pl.BlockSpec((slices, block_rows, bin_count), lambda i: (0, i, 0)),
        cost_estimate=pl.CostEstimate(flops=10**8, bytes_accessed=10**7, transcendentals=0),
        compiler_params=pltpu.CompilerParams(vmem_limit_bytes=24 * 2**20),
    )(place, turned, other_core(turned))


def solution(mesh):
    placed = (P(None, "ang", None), P("ang", None), P())
    return jax.shard_map(
        body, mesh=mesh, in_specs=placed, out_specs=P(None, "ang", None), check_vma=False
    )
```
